1024 devices in a mesh: fsdp: 64 (over z_hi, x, y), seq: 16 (over z_lo, core).
Axes of the slice: x: 4, y: 4, z: 32 (z_hi: 4, z_lo: 8; z = z_hi * 8 + z_lo), core: 2. Of those that a mesh axis runs over, the one named last changes fastest.
Arguments:
- tokens: bfloat16 [65536, 2304], P('fsdp', 'seq'), may hold values from -70 to 70
- gain: float32 [2304], replicated, may hold values from 0.1 to 1.9
- w_query: bfloat16 [2304, 4096], P('fsdp', 'seq'), may hold values from -3 to 3
- w_key: bfloat16 [2304, 2048], P('fsdp', 'seq'), may hold values from -3 to 3
- w_value: bfloat16 [2304, 2048], P('fsdp', 'seq'), may hold values from -0.125 to 0.125
Outputs:
- context: bfloat16 [65536, 4096], P('fsdp', 'seq')
The draws below stay inside these ranges and needn't reach their ends.
All inputs are finite; a program needn't handle non-finite values.
Results may differ from the reference program's by a relative error of at most 0.012.
The reference program's roundings to bfloat16 on the way (of `normed`, `values` and `weights`) count: a program that leaves them out, or rounds other values in their place, can miss the bound.
Values may be sent and summed in bfloat16 or wider, within the bound.
No kernel may reach another device: no remote copies, remote signals or barrier semaphores. Data moves between devices by JAX's collectives and lax.ppermute only.
A program may use at most 64 MiB of HBM per device.

```python
import math
import jax
import jax.numpy as jnp
from jax import lax

D = 2304
HEADS = 32
KV_HEADS = 16
HEAD_DIM = 128
SEQ_LEN = 1024
SEQS = 64


def draw_tokens(key, part):
    base_key, row_key, col_key = jax.random.split(jax.random.fold_in(key, 7), 3)
    count = SEQS * SEQ_LEN
    position = jnp.arange(D, dtype=jnp.float32) / D
    spread = math.log(10.0) * 0.5
    row_scale = jnp.exp(jax.random.uniform(row_key, (count, 1), jnp.float32, -spread, spread))
    col_scale = jnp.exp(jax.random.uniform(col_key, (1, D), jnp.float32, -spread, spread))
    base = jax.random.truncated_normal(base_key, -4.0, 4.0, (count, D), jnp.float32)
    ramp = jnp.exp(0.5 * math.log(3.0) * position)
    return (base * row_scale * col_scale * ramp[None, :]).astype(jnp.bfloat16)


def draw_w_query(key, part):
    base_key, scale_key = jax.random.split(jax.random.fold_in(key, 101))
    base = jax.random.truncated_normal(base_key, -4.0, 4.0, (D, HEADS * HEAD_DIM), jnp.float32)
    log_scale = jax.random.uniform(scale_key, (HEADS,), jnp.float32, 0.0, math.log(6.0))
    column_scale = jnp.repeat(jnp.exp(log_scale), HEAD_DIM)
    return (base * column_scale[None, :] / math.sqrt(D)).astype(jnp.bfloat16)


def draw_w_key(key, part):
    base_key, scale_key = jax.random.split(jax.random.fold_in(key, 202))
    base = jax.random.truncated_normal(base_key, -4.0, 4.0, (D, KV_HEADS * HEAD_DIM), jnp.float32)
    log_scale = jax.random.uniform(scale_key, (KV_HEADS,), jnp.float32, 0.0, math.log(6.0))
    column_scale = jnp.repeat(jnp.exp(log_scale), HEAD_DIM)
    return (base * column_scale[None, :] / math.sqrt(D)).astype(jnp.bfloat16)


def steps_of(own_key, shape, shards, least, top_value):
    def one(dim, blocks):
        heights = jax.random.uniform(jax.random.fold_in(jax.random.fold_in(own_key, 6), dim), (blocks,), jnp.float32, least / len(shards), top_value / len(shards))
        return jnp.repeat(jnp.exp(heights), shape[dim] // blocks).reshape((-1,) + (1,) * (len(shape) - dim - 1))

    loudness = one(*shards[0])
    for cut in shards[1:]:
        loudness = loudness * one(*cut)
    return loudness


def gaussian(rng, extent, scale, bound, cuts=(), held_as=jnp.bfloat16):
    values = scale * jax.random.normal(rng, extent, jnp.float32)
    if cuts:
        values = values * steps_of(rng, extent, cuts, -0.22, 0.18)
    return jnp.clip(values, -bound, bound).astype(held_as)


def setup_inputs(seed: int = 0) -> dict:
    arg_keys = jax.random.split(jax.random.key(seed), 6)
    return {
        "tokens": draw_tokens(jax.random.fold_in(arg_keys[5], 71), 0),
        "gain": jnp.clip(1.0 + 0.18 * jax.random.normal(arg_keys[1], (D,), jnp.float32), 0.1, 1.9),
        "w_query": draw_w_query(jax.random.fold_in(arg_keys[5], 71), 0),
        "w_key": draw_w_key(jax.random.fold_in(arg_keys[5], 71), 0),
        "w_value": gaussian(arg_keys[4], (D, KV_HEADS * HEAD_DIM), D ** -0.5, 0.125, ((0, 64), (1, 16))),
    }


def rotate(values, positions):
    half = values.shape[-1] // 2
    index = jnp.arange(half, dtype=jnp.float32)
    freqs = jnp.power(jnp.float32(10000.0), -2.0 * index / values.shape[-1])
    angle = positions[:, None] * freqs[None, :]
    cosine = jnp.cos(angle)[:, None, :]
    sine = jnp.sin(angle)[:, None, :]
    first = values[..., :half]
    second = values[..., half:]
    return jnp.concatenate([first * cosine - second * sine, second * cosine + first * sine], axis=-1)

def one_sequence(rows, gain, w_query, w_key, w_value):
    length = rows.shape[0]
    groups = HEADS // KV_HEADS
    floats = rows.astype(jnp.float32)
    inv_rms = lax.rsqrt(lax.optimization_barrier(jnp.mean(floats * floats, axis=-1, keepdims=True)) + 1e-06)
    normed = (floats * inv_rms * gain[None, :]).astype(jnp.bfloat16)
    positions = jnp.arange(length, dtype=jnp.float32)
    query_raw = jnp.dot(normed, w_query, preferred_element_type=jnp.float32).reshape(length, HEADS, HEAD_DIM)
    key_raw = jnp.dot(normed, w_key, preferred_element_type=jnp.float32).reshape(length, KV_HEADS, HEAD_DIM)
    values = jnp.dot(normed, w_value, preferred_element_type=jnp.float32).astype(jnp.bfloat16).reshape(length, KV_HEADS, HEAD_DIM)
    query = rotate(query_raw, positions).astype(jnp.bfloat16).reshape(length, KV_HEADS, groups, HEAD_DIM)
    keys = rotate(key_raw, positions).astype(jnp.bfloat16)
    scale = 1.0 / jnp.sqrt(jnp.float32(144.0))
    scores = jnp.einsum('lgqd,mgd->gqlm', query.astype(jnp.float32), keys.astype(jnp.float32)) * scale
    capped = 50.0 * jnp.tanh(scores / 50.0)
    causal = jnp.arange(length)[None, :] <= jnp.arange(length)[:, None]
    expo = jnp.where(causal[None, None], jnp.exp(capped), 0.0)
    weights = (expo / lax.optimization_barrier(jnp.sum(expo, axis=-1, keepdims=True))).astype(jnp.bfloat16)
    context = jnp.einsum('gqlm,mgd->lgqd', weights.astype(jnp.float32), values.astype(jnp.float32))
    return context.reshape(length, HEADS * HEAD_DIM).astype(jnp.bfloat16)

def reference(tokens, gain, w_query, w_key, w_value):
    seq_len = tokens.shape[0] // SEQS
    stacked = tokens.reshape(SEQS, seq_len, D)
    result = lax.map(lambda rows: one_sequence(rows, gain, w_query, w_key, w_value), stacked)
    return result.reshape(SEQS * seq_len, HEADS * HEAD_DIM)
```

```python
import jax
import jax.numpy as jnp
import numpy as np
from jax import lax
from jax.experimental import pallas as pl
from jax.experimental.pallas import tpu as pltpu
from jax.sharding import Mesh, PartitionSpec as P

HEAD_DIM = 128
HALF = 64
ROWS = 256
CHIPS = 8
FOLD = (0, 2, 4, 6, 7, 5, 3, 1)
CAP = 50.0
IN_SCALE = float(1.0 / (12.0 * 50.0))
OUT_SCALE = float(50.0 * np.log2(np.e))


def dot(a, b):
    return jnp.dot(a, b, preferred_element_type=jnp.float32)


def attend(place_ref, own_ref, other_ref, w0_ref, w3_ref, w1_ref, w2_ref, gain_ref, cos_ref, sin_ref,
           out_ref, w_ref, wt_ref, normed_ref, keys_ref, values_ref, weights_ref):
    block = pl.program_id(0)
    core = place_ref[0]
    here_x = place_ref[1]
    shard = own_ref.shape[1]
    width = 2 * CHIPS * shard

    @pl.when(block == 0)
    def _():
        depth = w0_ref.shape[0]
        for step, piece_ref in enumerate((w0_ref, w1_ref, w2_ref, w3_ref)):
            w_ref[step * depth : (step + 1) * depth, :] = piece_ref[...]
        wt_ref[...] = w_ref[...].T

    squares = jnp.zeros((shard, ROWS), jnp.float32)
    for ref in (own_ref, other_ref):
        for k in range(CHIPS):
            piece = ref[k].astype(jnp.float32)
            squares += piece * piece
    mean = jnp.sum(squares, axis=0, keepdims=True) * (1.0 / width)
    inv_rms = lax.rsqrt(mean + 1e-06)
    for ref, side in ((own_ref, core), (other_ref, 1 - core)):
        for k, chip in enumerate(FOLD):
            step = lax.rem((chip % 2) * 2 + side + 4 - here_x, 4)
            at = (step * 4 + chip // 2) * shard
            scaled = ref[k].astype(jnp.float32) * inv_rms * gain_ref[2 * chip + side]
            normed_ref[pl.ds(pl.multiple_of(at, 16), shard), :] = scaled.astype(jnp.bfloat16)

    raw = dot(wt_ref[...], normed_ref[...])
    cosine = cos_ref[...]
    sine = sin_ref[...]

    def rotate(at):
        a = raw[at : at + HALF]
        b = raw[at + HALF : at + HEAD_DIM]
        return jnp.concatenate([a * cosine - b * sine, b * cosine + a * sine], axis=0)

    query = jnp.concatenate([rotate(0), rotate(HEAD_DIM)], axis=1).astype(jnp.bfloat16)
    here = pl.ds(pl.multiple_of(block * ROWS, ROWS), ROWS)
    keys_ref[here, :] = rotate(2 * HEAD_DIM).T.astype(jnp.bfloat16)
    values_ref[block] = raw[3 * HEAD_DIM :].astype(jnp.bfloat16)

    def exponents(i):
        rows = pl.ds(pl.multiple_of(i * ROWS, ROWS), ROWS)
        scores = dot(keys_ref[rows, :], query)
        return jnp.exp2(jnp.tanh(scores * IN_SCALE) * OUT_SCALE)

    def first(i, total):
        part = exponents(i)
        weights_ref[i] = part
        return total + jnp.sum(part, axis=0, keepdims=True)

    key_at = lax.broadcasted_iota(jnp.int32, (ROWS, 2 * ROWS), 0)
    query_at = lax.broadcasted_iota(jnp.int32, (ROWS, 2 * ROWS), 1) % ROWS
    last = jnp.where(key_at <= query_at, exponents(block), 0.0)
    total = jnp.sum(last, axis=0, keepdims=True)
    total = lax.fori_loop(0, block, first, total)
    share = 1.0 / total

    def second(i, acc):
        part = (weights_ref[i] * share).astype(jnp.bfloat16)
        return acc + dot(values_ref[i], part)

    acc = dot(values_ref[block], (last * share).astype(jnp.bfloat16))
    acc = lax.fori_loop(0, block, second, acc)
    out_ref[:, :HEAD_DIM] = acc[:, :ROWS].T.astype(jnp.bfloat16)
    out_ref[:, HEAD_DIM:] = acc[:, ROWS:].T.astype(jnp.bfloat16)


def tables(length):
    index = jnp.arange(HALF, dtype=jnp.float32)
    freqs = jnp.power(jnp.float32(10000.0), -2.0 * index / HEAD_DIM)
    angle = freqs[:, None] * jnp.arange(length, dtype=jnp.float32)[None, :]
    return jnp.cos(angle), jnp.sin(angle)


def block_attention(place, own, other, w, gain, cosine, sine):
    chips, shard, length = own.shape
    depth, columns = w[0].shape
    width = 4 * depth
    blocks = length // ROWS
    x_spec = pl.BlockSpec((chips, shard, ROWS), lambda i, c: (0, 0, i))
    table_spec = pl.BlockSpec((HALF, ROWS), lambda i, c: (0, i))
    return pl.pallas_call(
        attend,
        out_shape=jax.ShapeDtypeStruct((length, columns // 2), jnp.bfloat16),
        grid_spec=pltpu.PrefetchScalarGridSpec(
            num_scalar_prefetch=1,
            grid=(blocks,),
            in_specs=[
                x_spec,
                x_spec,
                *[pl.BlockSpec((depth, columns), lambda i, c: (0, 0))] * 4,
                pl.BlockSpec((2 * chips, shard, 1), lambda i, c: (0, 0, 0)),
                table_spec,
                table_spec,
            ],
            out_specs=pl.BlockSpec((ROWS, columns // 2), lambda i, c: (i, 0)),
            scratch_shapes=[
                pltpu.VMEM((width, columns), jnp.bfloat16),
                pltpu.VMEM((columns, width), jnp.bfloat16),
                pltpu.VMEM((width, ROWS), jnp.bfloat16),
                pltpu.VMEM((length, HEAD_DIM), jnp.bfloat16),
                pltpu.VMEM((blocks, HEAD_DIM, ROWS), jnp.bfloat16),
                pltpu.VMEM((blocks, ROWS, 2 * ROWS), jnp.float32),
            ],
        ),
        compiler_params=pltpu.CompilerParams(
            dimension_semantics=("arbitrary",), vmem_limit_bytes=48 << 20
        ),
        name="attend",
    )(place, own, other, *w, gain, cosine, sine)


def local(tokens, gain, w_query, w_key, w_value):
    length, shard = tokens.shape
    run = [[z * 2 + c for z in FOLD] for c in range(2)]
    own = lax.all_gather(tokens.T, ("zl", "c"), axis=0, axis_index_groups=run)

    piece = jnp.concatenate([w_query, w_key, w_value], axis=1)
    rows, columns = piece.shape
    w = lax.all_gather(piece, "zh", axis=0, axis_index_groups=[[0, 1], [2, 3]])
    w = lax.all_gather(w, "zh", axis=0, axis_index_groups=[[0, 3], [1, 2]])
    w = lax.all_gather(w.reshape(4 * rows, columns), "y", axis=0)
    w = w.reshape(4, 4, rows, columns).transpose(1, 0, 2, 3).reshape(16 * rows, columns)
    core = lax.axis_index("c")
    behind = lax.ppermute(w, "x", [(i, (i + 1) % 4) for i in range(4)])
    ahead = lax.ppermute(w, "x", [(i, (i - 1) % 4) for i in range(4)])
    passed, own = lax.optimization_barrier((jnp.where(core == 0, behind, ahead), own))
    across = lax.ppermute(
        passed,
        ("x", "c"),
        [(i * 2 + c, (i + 1 - 2 * c) % 4 * 2 + c) for i in range(4) for c in range(2)],
    )

    other = lax.ppermute(own, "c", [(0, 1), (1, 0)])
    place = jnp.stack([core, lax.axis_index("x")]).astype(jnp.int32)
    cosine, sine = tables(length)
    pieces = (w, behind, ahead, across)
    return block_attention(place, own, other, pieces, gain.reshape(16, shard, 1), cosine, sine)


def solution(mesh):
    fine = Mesh(mesh.devices.reshape(4, 4, 4, 8, 2), ("zh", "x", "y", "zl", "c"))
    split = P(("zh", "x", "y"), ("zl", "c"))
    in_specs = (split, P(), split, split, split)
    return jax.shard_map(local, mesh=fine, in_specs=in_specs, out_specs=split, check_vma=False)
```

```python
import jax
import jax.numpy as jnp
import numpy as np
from jax import lax
from jax.experimental import pallas as pl
from jax.experimental.pallas import tpu as pltpu
from jax.sharding import Mesh, PartitionSpec as P

HEAD_DIM = 128
HALF = 64
ROWS = 256
CHIPS = 8
FOLD = (0, 2, 4, 6, 7, 5, 3, 1)
IN_SCALE = float(1.0 / (12.0 * 50.0))
OUT_SCALE = float(50.0 * np.log2(np.e))


def dot(a, b):
    return jnp.dot(a, b, preferred_element_type=jnp.float32)


def sum_squares(ref, i):
    shard, rows = ref.shape[2:]
    total = jnp.zeros((8, rows), jnp.float32)
    for k in range(CHIPS):
        piece = ref[k, i].astype(jnp.float32)
        total += jnp.sum((piece * piece).reshape(shard // 8, 8, rows), axis=0)
    return total


def turn(w0_ref, w3_ref, w1_ref, w2_ref, wt_ref, w_ref):
    depth = w0_ref.shape[0]
    for step, piece_ref in enumerate((w0_ref, w1_ref, w2_ref, w3_ref)):
        w_ref[step * depth : (step + 1) * depth, :] = piece_ref[...]
    wt_ref[...] = w_ref[...].T


def square(x_ref, out_ref):
    for i in range(x_ref.shape[1]):
        out_ref[:, i * ROWS : (i + 1) * ROWS] = sum_squares(x_ref, i)


def attend(place_ref, own_ref, other_hbm, squares_ref, wt_ref, gain_ref, cos_ref, sin_ref, out_hbm,
           other_ref, out_ref, normed_ref, keys_ref, values_ref, exps_ref, weights_ref, in_sems, out_sems):
    core = place_ref[0]
    here_x = place_ref[1]
    shard = own_ref.shape[2]
    blocks = own_ref.shape[1]
    width = 2 * CHIPS * shard
    copies = []
    for i in range(blocks):
        part = (slice(None), slice(i, i + 1))
        copies.append(pltpu.make_async_copy(other_hbm.at[part], other_ref.at[part], in_sems.at[i]))
    for copy in copies:
        copy.start()

    def norm(i):
        copies[i].wait()
        squares = squares_ref[:, i * ROWS : (i + 1) * ROWS] + sum_squares(other_ref, i)
        mean = jnp.sum(squares, axis=0, keepdims=True) * (1.0 / width)
        inv_rms = lax.rsqrt(mean + 1e-06)
        for ref, side in ((own_ref, core), (other_ref, 1 - core)):
            for k, chip in enumerate(FOLD):
                step = lax.rem((chip % 2) * 2 + side + 4 - here_x, 4)
                at = (step * 4 + chip // 2) * shard
                gain = gain_ref[2 * chip + side]
                gain = jnp.concatenate([gain] * (ROWS // 128), axis=1)
                scaled = ref[k, i].astype(jnp.float32) * inv_rms * gain
                normed_ref[i % 2, pl.ds(pl.multiple_of(at, 16), shard), :] = scaled.astype(
                    jnp.bfloat16
                )

    key_at = lax.broadcasted_iota(jnp.int32, (ROWS, 2 * ROWS), 0)
    query_at = lax.broadcasted_iota(jnp.int32, (ROWS, 2 * ROWS), 1) % ROWS
    results = []
    norm(0)
    for i in range(blocks):
        half = wt_ref.shape[0] // 2
        raw = jnp.concatenate(
            [dot(wt_ref[:half, :], normed_ref[i % 2]), dot(wt_ref[half:, :], normed_ref[i % 2])],
            axis=0,
        )
        if i + 1 < blocks:
            norm(i + 1)
        here = slice(i * ROWS, (i + 1) * ROWS)
        cosine = cos_ref[:, here]
        sine = sin_ref[:, here]

        def rotate(at):
            a = raw[at : at + HALF]
            b = raw[at + HALF : at + HEAD_DIM]
            return jnp.concatenate([a * cosine - b * sine, b * cosine + a * sine], axis=0)

        query = jnp.concatenate([rotate(0), rotate(HEAD_DIM)], axis=1).astype(jnp.bfloat16)
        keys_ref[here, :] = rotate(2 * HEAD_DIM).T.astype(jnp.bfloat16)
        values_ref[:, here] = raw[3 * HEAD_DIM :].astype(jnp.bfloat16)
        total = jnp.zeros((8, 2 * ROWS), jnp.float32)
        for b in range(i + 1):
            rows = slice(b * ROWS, (b + 1) * ROWS)
            scores = dot(keys_ref[rows, :], query)
            part = jnp.exp2(jnp.tanh(scores * IN_SCALE) * OUT_SCALE)
            if b == i:
                part = jnp.where(key_at <= query_at, part, 0.0)
            exps_ref[rows, :] = part
            total += jnp.sum(part.reshape(ROWS // 8, 8, 2 * ROWS), axis=0)
        share = 1.0 / jnp.sum(total, axis=0, keepdims=True)
        extent = (i + 1) * ROWS
        for b in range(i + 1):
            rows = slice(b * ROWS, (b + 1) * ROWS)
            weights_ref[rows, :] = (exps_ref[rows, :] * share).astype(jnp.bfloat16)
        acc = dot(values_ref[:, :extent], weights_ref[:extent, :])
        out_ref[here, :HEAD_DIM] = acc[:, :ROWS].T.astype(jnp.bfloat16)
        out_ref[here, HEAD_DIM:] = acc[:, ROWS:].T.astype(jnp.bfloat16)
        results.append(pltpu.make_async_copy(out_ref.at[here], out_hbm.at[here], out_sems.at[i]))
        results[i].start()
    for result in results:
        result.wait()


def tables(length):
    index = jnp.arange(HALF, dtype=jnp.float32)
    freqs = jnp.power(jnp.float32(10000.0), -2.0 * index / HEAD_DIM)
    angle = freqs[:, None] * jnp.arange(length, dtype=jnp.float32)[None, :]
    return jnp.cos(angle), jnp.sin(angle)


def turned(w):
    depth, columns = w[0].shape
    return pl.pallas_call(
        turn,
        out_shape=jax.ShapeDtypeStruct((columns, 4 * depth), jnp.bfloat16),
        in_specs=[pl.BlockSpec(memory_space=pltpu.VMEM)] * 4,
        out_specs=pl.BlockSpec(memory_space=pltpu.VMEM),
        scratch_shapes=[pltpu.VMEM((4 * depth, columns), jnp.bfloat16)],
        name="turn",
    )(*w)


def squared(x):
    chips, blocks, shard, rows = x.shape
    return pl.pallas_call(
        square,
        out_shape=jax.ShapeDtypeStruct((8, blocks * rows), jnp.float32),
        in_specs=[pl.BlockSpec(memory_space=pltpu.VMEM)],
        out_specs=pl.BlockSpec(memory_space=pltpu.VMEM),
        name="square",
    )(x)


def block_attention(place, own, other, squares, wt, gain, cosine, sine):
    chips, blocks, shard, rows = own.shape
    columns, width = wt.shape
    length = blocks * rows
    whole = pl.BlockSpec(memory_space=pltpu.VMEM)
    raw = pl.BlockSpec(memory_space=pl.ANY)
    return pl.pallas_call(
        attend,
        out_shape=jax.ShapeDtypeStruct((length, columns // 2), jnp.bfloat16),
        in_specs=[
            pl.BlockSpec(memory_space=pltpu.SMEM),
            whole,
            raw,
            whole,
            whole,
            whole,
            whole,
            whole,
        ],
        out_specs=raw,
        scratch_shapes=[
            pltpu.VMEM(own.shape, jnp.bfloat16),
            pltpu.VMEM((length, columns // 2), jnp.bfloat16),
            pltpu.VMEM((2, width, rows), jnp.bfloat16),
            pltpu.VMEM((length, HEAD_DIM), jnp.bfloat16),
            pltpu.VMEM((HEAD_DIM, length), jnp.bfloat16),
            pltpu.VMEM((length, 2 * rows), jnp.float32),
            pltpu.VMEM((length, 2 * rows), jnp.bfloat16),
            pltpu.SemaphoreType.DMA((blocks,)),
            pltpu.SemaphoreType.DMA((blocks,)),
        ],
        compiler_params=pltpu.CompilerParams(vmem_limit_bytes=48 << 20),
        name="attend",
    )(place, own, other, squares, wt, gain, cosine, sine)


def local(tokens, gain, w_query, w_key, w_value):
    length, shard = tokens.shape
    run = [[z * 2 + c for z in FOLD] for c in range(2)]
    blocks = tokens.T.reshape(shard, length // ROWS, ROWS).transpose(1, 0, 2)
    own = lax.all_gather(blocks, ("zl", "c"), axis=0, axis_index_groups=run)

    piece = jnp.concatenate([w_query, w_key, w_value], axis=1)
    rows, columns = piece.shape
    w = lax.all_gather(piece, "zh", axis=0)
    w = lax.all_gather(w.reshape(4 * rows, columns), "y", axis=0)
    w = w.reshape(4, 4, rows, columns).transpose(1, 0, 2, 3).reshape(16 * rows, columns)
    core = lax.axis_index("c")
    behind = lax.ppermute(w, "x", [(i, (i + 1) % 4) for i in range(4)])
    ahead = lax.ppermute(w, "x", [(i, (i - 1) % 4) for i in range(4)])
    across = lax.ppermute(
        jnp.where(core == 0, behind, ahead),
        ("x", "c"),
        [(i * 2 + c, (i + 1 - 2 * c) % 4 * 2 + c) for i in range(4) for c in range(2)],
    )
    wt = turned((w, behind, ahead, across))

    wt, own = lax.optimization_barrier((wt, own))
    other = lax.ppermute(own, "c", [(0, 1), (1, 0)])
    squares = squared(own)
    place = jnp.stack([core, lax.axis_index("x")]).astype(jnp.int32)
    cosine, sine = tables(length)
    wide = jnp.broadcast_to(gain.reshape(16, shard, 1), (16, shard, 128))
    return block_attention(place, own, other, squares, wt, wide, cosine, sine)


def solution(mesh):
    fine = Mesh(mesh.devices.reshape(4, 4, 4, 8, 2), ("zh", "x", "y", "zl", "c"))
    split = P(("zh", "x", "y"), ("zl", "c"))
    in_specs = (split, P(), split, split, split)
    return jax.shard_map(local, mesh=fine, in_specs=in_specs, out_specs=split, check_vma=False)
```

```python
import jax
import jax.numpy as jnp
import numpy as np
from jax import lax
from jax.experimental import pallas as pl
from jax.experimental.pallas import tpu as pltpu
from jax.sharding import Mesh, PartitionSpec as P


HEAD_DIM = 128
HALF = 64
ROWS = 256
CHIPS = 8
FOLD = (0, 2, 4, 6, 7, 5, 3, 1)
IN_SCALE = float(1.0 / (12.0 * 50.0))
OUT_SCALE = float(50.0 * np.log2(np.e))


def dot(a, b):
    return jnp.dot(a, b, preferred_element_type=jnp.float32)


def sum_squares(ref, here):
    shard = ref.shape[1]
    total = jnp.zeros((8, ROWS), jnp.float32)
    for k in range(CHIPS):
        piece = ref[k, :, here].astype(jnp.float32)
        total += jnp.sum((piece * piece).reshape(shard // 8, 8, ROWS), axis=0)
    return total


def turn(w0_ref, w3_ref, w1_ref, w2_ref, wt_ref, w_ref):
    depth = w0_ref.shape[0]
    for step, piece_ref in enumerate((w0_ref, w1_ref, w2_ref, w3_ref)):
        w_ref[step * depth : (step + 1) * depth, :] = piece_ref[...]
    wt_ref[...] = w_ref[...].T


def square(x_ref, out_ref):
    for i in range(x_ref.shape[2] // ROWS):
        here = slice(i * ROWS, (i + 1) * ROWS)
        out_ref[:, here] = sum_squares(x_ref, here)


def attend(place_ref, own_ref, other_hbm, squares_ref, wt_ref, gain_ref, cos_ref, sin_ref, out_hbm,
           other_ref, out_ref, normed_ref, keys_ref, values_ref, exps_ref, weights_ref, in_sems, out_sems):
    core = place_ref[0]
    here_x = place_ref[1]
    shard = own_ref.shape[1]
    blocks = own_ref.shape[2] // ROWS
    width = 2 * CHIPS * shard
    copies = []
    for i in range(blocks):
        part = (slice(None), slice(None), slice(i * ROWS, (i + 1) * ROWS))
        copies.append(pltpu.make_async_copy(other_hbm.at[part], other_ref.at[part], in_sems.at[i]))
    for copy in copies:
        copy.start()

    def norm(i):
        copies[i].wait()
        here = slice(i * ROWS, (i + 1) * ROWS)
        squares = squares_ref[:, here] + sum_squares(other_ref, here)
        mean = jnp.sum(squares, axis=0, keepdims=True) * (1.0 / width)
        inv_rms = lax.rsqrt(mean + 1e-06)
        for ref, side in ((own_ref, core), (other_ref, 1 - core)):
            for k, chip in enumerate(FOLD):
                step = lax.rem((chip % 2) * 2 + side + 4 - here_x, 4)
                at = (step * 4 + chip // 2) * shard
                gain = gain_ref[2 * chip + side]
                gain = jnp.concatenate([gain] * (ROWS // 128), axis=1)
                scaled = ref[k, :, here].astype(jnp.float32) * inv_rms * gain
                normed_ref[i % 2, pl.ds(pl.multiple_of(at, 16), shard), :] = scaled.astype(
                    jnp.bfloat16
                )

    key_at = lax.broadcasted_iota(jnp.int32, (ROWS, 2 * ROWS), 0)
    query_at = lax.broadcasted_iota(jnp.int32, (ROWS, 2 * ROWS), 1) % ROWS
    results = []
    norm(0)
    for i in range(blocks):
        half = wt_ref.shape[0] // 2
        raw = jnp.concatenate(
            [dot(wt_ref[:half, :], normed_ref[i % 2]), dot(wt_ref[half:, :], normed_ref[i % 2])],
            axis=0,
        )
        if i + 1 < blocks:
            norm(i + 1)
        here = slice(i * ROWS, (i + 1) * ROWS)
        cosine = cos_ref[:, here]
        sine = sin_ref[:, here]

        def rotate(at):
            a = raw[at : at + HALF]
            b = raw[at + HALF : at + HEAD_DIM]
            return jnp.concatenate([a * cosine - b * sine, b * cosine + a * sine], axis=0)

        query = jnp.concatenate([rotate(0), rotate(HEAD_DIM)], axis=1).astype(jnp.bfloat16)
        keys_ref[here, :] = rotate(2 * HEAD_DIM).T.astype(jnp.bfloat16)
        values_ref[:, here] = raw[3 * HEAD_DIM :].astype(jnp.bfloat16)
        total = jnp.zeros((8, 2 * ROWS), jnp.float32)
        for b in range(i + 1):
            rows = slice(b * ROWS, (b + 1) * ROWS)
            scores = dot(keys_ref[rows, :], query)
            part = jnp.exp2(jnp.tanh(scores * IN_SCALE) * OUT_SCALE)
            if b == i:
                part = jnp.where(key_at <= query_at, part, 0.0)
            exps_ref[rows, :] = part
            total += jnp.sum(part.reshape(ROWS // 8, 8, 2 * ROWS), axis=0)
        share = 1.0 / jnp.sum(total, axis=0, keepdims=True)
        extent = (i + 1) * ROWS
        for b in range(i + 1):
            rows = slice(b * ROWS, (b + 1) * ROWS)
            weights_ref[rows, :] = (exps_ref[rows, :] * share).astype(jnp.bfloat16)
        acc = dot(values_ref[:, :extent], weights_ref[:extent, :])
        out_ref[here, :HEAD_DIM] = acc[:, :ROWS].T.astype(jnp.bfloat16)
        out_ref[here, HEAD_DIM:] = acc[:, ROWS:].T.astype(jnp.bfloat16)
        results.append(pltpu.make_async_copy(out_ref.at[here], out_hbm.at[here], out_sems.at[i]))
        results[i].start()
    for result in results:
        result.wait()


def tables(length):
    index = jnp.arange(HALF, dtype=jnp.float32)
    freqs = jnp.power(jnp.float32(10000.0), -2.0 * index / HEAD_DIM)
    angle = freqs[:, None] * jnp.arange(length, dtype=jnp.float32)[None, :]
    return jnp.cos(angle), jnp.sin(angle)


def turned(w):
    depth, columns = w[0].shape
    return pl.pallas_call(
        turn,
        out_shape=jax.ShapeDtypeStruct((columns, 4 * depth), jnp.bfloat16),
        in_specs=[pl.BlockSpec(memory_space=pltpu.VMEM)] * 4,
        out_specs=pl.BlockSpec(memory_space=pltpu.VMEM),
        scratch_shapes=[pltpu.VMEM((4 * depth, columns), jnp.bfloat16)],
        compiler_params=pltpu.CompilerParams(vmem_limit_bytes=12 << 20),
        name="turn",
    )(*w)


def squared(x):
    length = x.shape[2]
    return pl.pallas_call(
        square,
        out_shape=jax.ShapeDtypeStruct((8, length), jnp.float32),
        in_specs=[pl.BlockSpec(memory_space=pltpu.VMEM)],
        out_specs=pl.BlockSpec(memory_space=pltpu.VMEM),
        compiler_params=pltpu.CompilerParams(vmem_limit_bytes=8 << 20),
        name="square",
    )(x)


def block_attention(place, own, other, squares, wt, gain, cosine, sine):
    length = own.shape[2]
    rows, blocks = ROWS, length // ROWS
    columns, width = wt.shape
    whole = pl.BlockSpec(memory_space=pltpu.VMEM)
    raw = pl.BlockSpec(memory_space=pl.ANY)
    return pl.pallas_call(
        attend,
        out_shape=jax.ShapeDtypeStruct((length, columns // 2), jnp.bfloat16),
        in_specs=[
            pl.BlockSpec(memory_space=pltpu.SMEM),
            whole,
            raw,
            whole,
            whole,
            whole,
            whole,
            whole,
        ],
        out_specs=raw,
        scratch_shapes=[
            pltpu.VMEM(own.shape, jnp.bfloat16),
            pltpu.VMEM((length, columns // 2), jnp.bfloat16),
            pltpu.VMEM((2, width, rows), jnp.bfloat16),
            pltpu.VMEM((length, HEAD_DIM), jnp.bfloat16),
            pltpu.VMEM((HEAD_DIM, length), jnp.bfloat16),
            pltpu.VMEM((length, 2 * rows), jnp.float32),
            pltpu.VMEM((length, 2 * rows), jnp.bfloat16),
            pltpu.SemaphoreType.DMA((blocks,)),
            pltpu.SemaphoreType.DMA((blocks,)),
        ],
        compiler_params=pltpu.CompilerParams(vmem_limit_bytes=24 << 20),
        name="attend",
    )(place, own, other, squares, wt, gain, cosine, sine)


def local(tokens, gain, w_query, w_key, w_value):
    length, shard = tokens.shape
    run = [[z * 2 + c for z in FOLD] for c in range(2)]
    own = lax.all_gather(tokens.T, ("zl", "c"), axis=0, axis_index_groups=run)

    piece = jnp.concatenate([w_query, w_key, w_value], axis=1)
    rows, columns = piece.shape
    w = lax.all_gather(piece, "zh", axis=0)
    w = lax.all_gather(w.reshape(4 * rows, columns), "y", axis=0)
    w = w.reshape(4, 4, rows, columns).transpose(1, 0, 2, 3).reshape(16 * rows, columns)
    core = lax.axis_index("c")
    behind = lax.ppermute(w, "x", [(i, (i + 1) % 4) for i in range(4)])
    ahead = lax.ppermute(w, "x", [(i, (i - 1) % 4) for i in range(4)])
    across = lax.ppermute(
        jnp.where(core == 0, behind, ahead),
        ("x", "c"),
        [(i * 2 + c, (i + 1 - 2 * c) % 4 * 2 + c) for i in range(4) for c in range(2)],
    )
    other = lax.ppermute(own, "c", [(0, 1), (1, 0)])
    squares = squared(own)
    wt = turned((w, behind, ahead, across))
    place = jnp.stack([core, lax.axis_index("x")]).astype(jnp.int32)
    cosine, sine = tables(length)
    wide = jnp.broadcast_to(gain.reshape(16, shard, 1), (16, shard, 128))
    return block_attention(place, own, other, squares, wt, wide, cosine, sine)


def solution(mesh):
    fine = Mesh(mesh.devices.reshape(4, 4, 4, 8, 2), ("zh", "x", "y", "zl", "c"))
    split = P(("zh", "x", "y"), ("zl", "c"))
    in_specs = (split, P(), split, split, split)

    return jax.shard_map(local, mesh=fine, in_specs=in_specs, out_specs=split, check_vma=False)
```

```python
import jax
import jax.numpy as jnp
import numpy as np
from jax import lax
from jax.experimental import pallas as pl
from jax.experimental.pallas import tpu as pltpu
from jax.sharding import Mesh, PartitionSpec as P


HEAD_DIM = 128
HALF = 64
ROWS = 256
CHIPS = 8
FOLD = (0, 2, 4, 6, 7, 5, 3, 1)
IN_SCALE = float(1.0 / (12.0 * 50.0))
OUT_SCALE = float(50.0 * np.log2(np.e))


def dot(a, b):
    return jnp.dot(a, b, preferred_element_type=jnp.float32)


def sum_squares(ref, here):
    shard = ref.shape[1]
    total = jnp.zeros((8, ROWS), jnp.float32)
    for k in range(CHIPS):
        piece = ref[k, :, here].astype(jnp.float32)
        total += jnp.sum((piece * piece).reshape(shard // 8, 8, ROWS), axis=0)
    return total


def turn(*refs):
    pieces, wt_ref, w_ref = refs[:-2], refs[-2], refs[-1]
    depth = pieces[0].shape[0]
    for at, piece_ref in enumerate(pieces):
        w_ref[at * depth : (at + 1) * depth, :] = piece_ref[...]
    wt_ref[...] = w_ref[...].T


def square(x_ref, out_ref):
    for i in range(x_ref.shape[2] // ROWS):
        here = slice(i * ROWS, (i + 1) * ROWS)
        out_ref[:, here] = sum_squares(x_ref, here)


def attend(place_ref, own_ref, other_any, squares_ref, near_ref, far_ref, gain_ref, cos_ref, sin_ref,
           out_hbm, other_ref, out_ref, normed_ref, keys_ref, values_ref, exps_ref, weights_ref, in_sems, out_sems):
    core = place_ref[0]
    here_x = place_ref[1]
    shard = own_ref.shape[1]
    blocks = own_ref.shape[2] // ROWS
    width = 2 * CHIPS * shard

    copies = []
    for i in range(blocks):
        part = (slice(None), slice(None), slice(i * ROWS, (i + 1) * ROWS))
        copies.append(pltpu.make_async_copy(other_any.at[part], other_ref.at[part], in_sems.at[i]))
    for copy in copies:
        copy.start()

    def norm(i):
        copies[i].wait()
        here = slice(i * ROWS, (i + 1) * ROWS)
        squares = squares_ref[:, here] + sum_squares(other_ref, here)
        mean = jnp.sum(squares, axis=0, keepdims=True) * (1.0 / width)
        inv_rms = lax.rsqrt(mean + 1e-06)
        for ref, side in ((own_ref, core), (other_ref, 1 - core)):
            for k, chip in enumerate(FOLD):
                step = lax.rem((chip % 2) * 2 + side + 4 - here_x, 4)
                place = step ^ (step >> 1)
                at = (place * 4 + chip // 2) * shard
                gain = gain_ref[2 * chip + side]
                gain = jnp.concatenate([gain] * (ROWS // 128), axis=1)
                scaled = ref[k, :, here].astype(jnp.float32) * inv_rms * gain
                normed_ref[i % 2, pl.ds(pl.multiple_of(at, 16), shard), :] = scaled.astype(
                    jnp.bfloat16
                )

    key_at = lax.broadcasted_iota(jnp.int32, (ROWS, 2 * ROWS), 0)
    query_at = lax.broadcasted_iota(jnp.int32, (ROWS, 2 * ROWS), 1) % ROWS
    results = []
    norm(0)
    for i in range(blocks):
        half = near_ref.shape[0] // 2
        cut = near_ref.shape[1]
        raw = jnp.concatenate(
            [
                dot(near_ref[rows, :], normed_ref[i % 2, :cut])
                + dot(far_ref[rows, :], normed_ref[i % 2, cut:])
                for rows in (slice(0, half), slice(half, 2 * half))
            ],
            axis=0,
        )
        if i + 1 < blocks:
            norm(i + 1)
        here = slice(i * ROWS, (i + 1) * ROWS)
        cosine = cos_ref[:, here]
        sine = sin_ref[:, here]

        def rotate(at):
            a = raw[at : at + HALF]
            b = raw[at + HALF : at + HEAD_DIM]
            return jnp.concatenate([a * cosine - b * sine, b * cosine + a * sine], axis=0)

        query = jnp.concatenate([rotate(0), rotate(HEAD_DIM)], axis=1).astype(jnp.bfloat16)
        keys_ref[here, :] = rotate(2 * HEAD_DIM).T.astype(jnp.bfloat16)
        values_ref[:, here] = raw[3 * HEAD_DIM :].astype(jnp.bfloat16)
        total = jnp.zeros((8, 2 * ROWS), jnp.float32)
        for b in range(i + 1):
            rows = slice(b * ROWS, (b + 1) * ROWS)
            scores = dot(keys_ref[rows, :], query)
            part = jnp.exp2(jnp.tanh(scores * IN_SCALE) * OUT_SCALE)
            if b == i:
                part = jnp.where(key_at <= query_at, part, 0.0)
            exps_ref[rows, :] = part
            total += jnp.sum(part.reshape(ROWS // 8, 8, 2 * ROWS), axis=0)
        share = 1.0 / jnp.sum(total, axis=0, keepdims=True)
        extent = (i + 1) * ROWS
        for b in range(i + 1):
            rows = slice(b * ROWS, (b + 1) * ROWS)
            weights_ref[rows, :] = (exps_ref[rows, :] * share).astype(jnp.bfloat16)
        acc = dot(values_ref[:, :extent], weights_ref[:extent, :])
        out_ref[here, :HEAD_DIM] = acc[:, :ROWS].T.astype(jnp.bfloat16)
        out_ref[here, HEAD_DIM:] = acc[:, ROWS:].T.astype(jnp.bfloat16)
        results.append(pltpu.make_async_copy(out_ref.at[here], out_hbm.at[here], out_sems.at[i]))
        results[i].start()
    for result in results:
        result.wait()


def tables(length):
    index = jnp.arange(HALF, dtype=jnp.float32)
    freqs = jnp.power(jnp.float32(10000.0), -2.0 * index / HEAD_DIM)
    angle = freqs[:, None] * jnp.arange(length, dtype=jnp.float32)[None, :]
    return jnp.cos(angle), jnp.sin(angle)


def turned(*w):
    depth, columns = w[0].shape
    width = len(w) * depth
    return pl.pallas_call(
        turn,
        out_shape=jax.ShapeDtypeStruct((columns, width), jnp.bfloat16),
        in_specs=[pl.BlockSpec(memory_space=pltpu.VMEM)] * len(w),
        out_specs=pl.BlockSpec(memory_space=pltpu.VMEM),
        scratch_shapes=[pltpu.VMEM((width, columns), jnp.bfloat16)],
        compiler_params=pltpu.CompilerParams(vmem_limit_bytes=8 << 20),
        name="turn",
    )(*w)


def squared(x):
    length = x.shape[2]
    return pl.pallas_call(
        square,
        out_shape=jax.ShapeDtypeStruct((8, length), jnp.float32),
        in_specs=[pl.BlockSpec(memory_space=pltpu.VMEM)],
        out_specs=pl.BlockSpec(memory_space=pltpu.VMEM),
        compiler_params=pltpu.CompilerParams(vmem_limit_bytes=8 << 20),
        name="square",
    )(x)


def block_attention(place, own, other, squares, near, far, gain, cosine, sine):
    length = own.shape[2]
    rows, blocks = ROWS, length // ROWS
    columns = near.shape[0]
    width = near.shape[1] + far.shape[1]
    whole = pl.BlockSpec(memory_space=pltpu.VMEM)
    raw = pl.BlockSpec(memory_space=pl.ANY)
    return pl.pallas_call(
        attend,
        out_shape=jax.ShapeDtypeStruct((length, columns // 2), jnp.bfloat16),
        in_specs=[
            pl.BlockSpec(memory_space=pltpu.SMEM),
            whole,
            raw,
            *[whole] * 6,
        ],
        out_specs=raw,
        scratch_shapes=[
            pltpu.VMEM(own.shape, jnp.bfloat16),
            pltpu.VMEM((length, columns // 2), jnp.bfloat16),
            pltpu.VMEM((2, width, rows), jnp.bfloat16),
            pltpu.VMEM((length, HEAD_DIM), jnp.bfloat16),
            pltpu.VMEM((HEAD_DIM, length), jnp.bfloat16),
            pltpu.VMEM((length, 2 * rows), jnp.float32),
            pltpu.VMEM((length, 2 * rows), jnp.bfloat16),
            pltpu.SemaphoreType.DMA((blocks,)),
            pltpu.SemaphoreType.DMA((blocks,)),
        ],
        compiler_params=pltpu.CompilerParams(vmem_limit_bytes=20 << 20),
        name="attend",
    )(place, own, other, squares, near, far, gain, cosine, sine)


def local(tokens, gain, w_query, w_key, w_value):
    length, shard = tokens.shape
    run = [[z * 2 + c for z in FOLD] for c in range(2)]
    own = lax.all_gather(tokens.T, ("zl", "c"), axis=0, axis_index_groups=run)

    piece = jnp.concatenate([w_query, w_key, w_value], axis=1)
    rows, columns = piece.shape
    w = lax.all_gather(piece, "zh", axis=0)
    w = lax.all_gather(w.reshape(4 * rows, columns), "y", axis=0)
    w = w.reshape(4, 4, rows, columns).transpose(1, 0, 2, 3).reshape(16 * rows, columns)
    core = lax.axis_index("c")
    behind = lax.ppermute(w, "x", [(i, (i + 1) % 4) for i in range(4)])
    ahead = lax.ppermute(w, "x", [(i, (i - 1) % 4) for i in range(4)])
    across = lax.ppermute(
        jnp.where(core == 0, behind, ahead),
        ("x", "c"),
        [(i * 2 + c, (i + 1 - 2 * c) % 4 * 2 + c) for i in range(4) for c in range(2)],
    )
    other = lax.ppermute(own, "c", [(0, 1), (1, 0)])
    squares = squared(own)
    near = turned(w, ahead, behind)
    far = turned(across)
    place = jnp.stack([core, lax.axis_index("x")]).astype(jnp.int32)
    cosine, sine = tables(length)
    wide = jnp.broadcast_to(gain.reshape(16, shard, 1), (16, shard, 128))
    return block_attention(place, own, other, squares, near, far, wide, cosine, sine)


def solution(mesh):
    fine = Mesh(mesh.devices.reshape(4, 4, 4, 8, 2), ("zh", "x", "y", "zl", "c"))
    split = P(("zh", "x", "y"), ("zl", "c"))
    in_specs = (split, P(), split, split, split)

    return jax.shard_map(local, mesh=fine, in_specs=in_specs, out_specs=split, check_vma=False)
```

```python
import jax
import jax.numpy as jnp
import numpy as np
from jax import lax
from jax.experimental import pallas as pl
from jax.experimental.pallas import tpu as pltpu
from jax.sharding import Mesh, PartitionSpec as P


HEAD_DIM = 128
HALF = 64
ROWS = 256
CHIPS = 8
FOLD = (0, 2, 4, 6, 7, 5, 3, 1)
IN_SCALE = float(1.0 / (12.0 * 50.0))
OUT_SCALE = float(50.0 * np.log2(np.e))


def dot(a, b):
    return jnp.dot(a, b, preferred_element_type=jnp.float32)


def sum_squares(ref, here):
    shard = ref.shape[1]
    total = jnp.zeros((8, ROWS), jnp.float32)
    for k in range(CHIPS):
        piece = ref[k, :, here].astype(jnp.float32)
        total += jnp.sum((piece * piece).reshape(shard // 8, 8, ROWS), axis=0)
    return total


def turn(*refs):
    pieces, wt_ref, w_ref = refs[:-2], refs[-2], refs[-1]
    depth = pieces[0].shape[0]
    for at, piece_ref in enumerate(pieces):
        w_ref[at * depth : (at + 1) * depth, :] = piece_ref[...]
    wt_ref[...] = w_ref[...].T


def square(x_ref, out_ref):
    for i in range(x_ref.shape[2] // ROWS):
        here = slice(i * ROWS, (i + 1) * ROWS)
        out_ref[:, here] = sum_squares(x_ref, here)


def attend(place_ref, own_ref, other_any, squares_ref, near_ref, far_ref, gain_ref, cos_ref, sin_ref,
           out_hbm, other_ref, out_ref, normed_ref, keys_ref, values_ref, exps_ref, weights_ref, in_sems, out_sems):
    core = place_ref[0]
    here_x = place_ref[1]
    shard = own_ref.shape[1]
    blocks = own_ref.shape[2] // ROWS
    width = 2 * CHIPS * shard

    copies = []
    for k in range(CHIPS):
        copies.append(pltpu.make_async_copy(other_any.at[k], other_ref.at[k], in_sems.at[k]))
    for copy in copies:
        copy.start()

    def norm(i):
        for copy in copies if i == 0 else ():
            copy.wait()
        here = slice(i * ROWS, (i + 1) * ROWS)
        squares = squares_ref[:, here] + sum_squares(other_ref, here)
        mean = jnp.sum(squares, axis=0, keepdims=True) * (1.0 / width)
        inv_rms = lax.rsqrt(mean + 1e-06)
        for ref, side in ((own_ref, core), (other_ref, 1 - core)):
            for k, chip in enumerate(FOLD):
                step = lax.rem((chip % 2) * 2 + side + 4 - here_x, 4)
                place = step ^ (step >> 1)
                at = (place * 4 + chip // 2) * shard
                gain = gain_ref[2 * chip + side]
                gain = jnp.concatenate([gain] * (ROWS // 128), axis=1)
                scaled = ref[k, :, here].astype(jnp.float32) * inv_rms * gain
                normed_ref[i % 2, pl.ds(pl.multiple_of(at, 16), shard), :] = scaled.astype(
                    jnp.bfloat16
                )

    key_at = lax.broadcasted_iota(jnp.int32, (ROWS, 2 * ROWS), 0)
    query_at = lax.broadcasted_iota(jnp.int32, (ROWS, 2 * ROWS), 1) % ROWS
    results = []
    norm(0)
    for i in range(blocks):
        half = near_ref.shape[0] // 2
        cut = near_ref.shape[1]
        raw = jnp.concatenate(
            [
                dot(near_ref[rows, :], normed_ref[i % 2, :cut])
                + dot(far_ref[rows, :], normed_ref[i % 2, cut:])
                for rows in (slice(0, half), slice(half, 2 * half))
            ],
            axis=0,
        )
        if i + 1 < blocks:
            norm(i + 1)
        here = slice(i * ROWS, (i + 1) * ROWS)
        cosine = cos_ref[:, here]
        sine = sin_ref[:, here]

        def rotate(at):
            a = raw[at : at + HALF]
            b = raw[at + HALF : at + HEAD_DIM]
            return jnp.concatenate([a * cosine - b * sine, b * cosine + a * sine], axis=0)

        query = jnp.concatenate([rotate(0), rotate(HEAD_DIM)], axis=1).astype(jnp.bfloat16)
        keys_ref[here, :] = rotate(2 * HEAD_DIM).T.astype(jnp.bfloat16)
        values_ref[:, here] = raw[3 * HEAD_DIM :].astype(jnp.bfloat16)
        total = jnp.zeros((8, 2 * ROWS), jnp.float32)
        for b in range(i + 1):
            rows = slice(b * ROWS, (b + 1) * ROWS)
            scores = dot(keys_ref[rows, :], query)
            part = jnp.exp2(jnp.tanh(scores * IN_SCALE) * OUT_SCALE)
            if b == i:
                part = jnp.where(key_at <= query_at, part, 0.0)
            exps_ref[rows, :] = part
            total += jnp.sum(part.reshape(ROWS // 8, 8, 2 * ROWS), axis=0)
        share = 1.0 / jnp.sum(total, axis=0, keepdims=True)
        extent = (i + 1) * ROWS
        for b in range(i + 1):
            rows = slice(b * ROWS, (b + 1) * ROWS)
            weights_ref[rows, :] = (exps_ref[rows, :] * share).astype(jnp.bfloat16)
        acc = dot(values_ref[:, :extent], weights_ref[:extent, :])
        out_ref[here, :HEAD_DIM] = acc[:, :ROWS].T.astype(jnp.bfloat16)
        out_ref[here, HEAD_DIM:] = acc[:, ROWS:].T.astype(jnp.bfloat16)
        results.append(pltpu.make_async_copy(out_ref.at[here], out_hbm.at[here], out_sems.at[i]))
        results[i].start()
    for result in results:
        result.wait()


def tables(length):
    index = jnp.arange(HALF, dtype=jnp.float32)
    freqs = jnp.power(jnp.float32(10000.0), -2.0 * index / HEAD_DIM)
    angle = freqs[:, None] * jnp.arange(length, dtype=jnp.float32)[None, :]
    return jnp.cos(angle), jnp.sin(angle)


def turned(*w):
    depth, columns = w[0].shape
    width = len(w) * depth
    return pl.pallas_call(
        turn,
        out_shape=jax.ShapeDtypeStruct((columns, width), jnp.bfloat16),
        in_specs=[pl.BlockSpec(memory_space=pltpu.VMEM)] * len(w),
        out_specs=pl.BlockSpec(memory_space=pltpu.VMEM),
        scratch_shapes=[pltpu.VMEM((width, columns), jnp.bfloat16)],
        compiler_params=pltpu.CompilerParams(vmem_limit_bytes=8 << 20),
        name="turn",
    )(*w)


def squared(x):
    length = x.shape[2]
    return pl.pallas_call(
        square,
        out_shape=jax.ShapeDtypeStruct((8, length), jnp.float32),
        in_specs=[pl.BlockSpec(memory_space=pltpu.VMEM)],
        out_specs=pl.BlockSpec(memory_space=pltpu.VMEM),
        compiler_params=pltpu.CompilerParams(vmem_limit_bytes=8 << 20),
        name="square",
    )(x)


def block_attention(place, own, other, squares, near, far, gain, cosine, sine):
    length = own.shape[2]
    rows, blocks = ROWS, length // ROWS
    columns = near.shape[0]
    width = near.shape[1] + far.shape[1]
    whole = pl.BlockSpec(memory_space=pltpu.VMEM)
    raw = pl.BlockSpec(memory_space=pl.ANY)
    return pl.pallas_call(
        attend,
        out_shape=jax.ShapeDtypeStruct((length, columns // 2), jnp.bfloat16),
        in_specs=[
            pl.BlockSpec(memory_space=pltpu.SMEM),
            whole,
            raw,
            *[whole] * 6,
        ],
        out_specs=raw,
        scratch_shapes=[
            pltpu.VMEM(own.shape, jnp.bfloat16),
            pltpu.VMEM((length, columns // 2), jnp.bfloat16),
            pltpu.VMEM((2, width, rows), jnp.bfloat16),
            pltpu.VMEM((length, HEAD_DIM), jnp.bfloat16),
            pltpu.VMEM((HEAD_DIM, length), jnp.bfloat16),
            pltpu.VMEM((length, 2 * rows), jnp.float32),
            pltpu.VMEM((length, 2 * rows), jnp.bfloat16),
            pltpu.SemaphoreType.DMA((CHIPS,)),
            pltpu.SemaphoreType.DMA((blocks,)),
        ],
        compiler_params=pltpu.CompilerParams(vmem_limit_bytes=20 << 20),
        cost_estimate=pl.CostEstimate(
            flops=2 * length * width * columns + 2 * length * length * columns,
            transcendentals=2 * length * length,
            bytes_accessed=2 * (2 * own.size + width * columns + length * columns // 2),
        ),
        name="attend",
    )(place, own, other, squares, near, far, gain, cosine, sine)


def local(tokens, gain, w_query, w_key, w_value):
    length, shard = tokens.shape
    run = [[z * 2 + c for z in FOLD] for c in range(2)]
    own = lax.all_gather(tokens.T, ("zl", "c"), axis=0, axis_index_groups=run)

    piece = jnp.concatenate([w_query, w_key, w_value], axis=1)
    rows, columns = piece.shape
    w = lax.all_gather(piece, "zh", axis=0)
    w = lax.all_gather(w.reshape(4 * rows, columns), "y", axis=0)
    w = w.reshape(4, 4, rows, columns).transpose(1, 0, 2, 3).reshape(16 * rows, columns)
    core = lax.axis_index("c")
    behind = lax.ppermute(w, "x", [(i, (i + 1) % 4) for i in range(4)])
    ahead = lax.ppermute(w, "x", [(i, (i - 1) % 4) for i in range(4)])
    across = lax.ppermute(
        jnp.where(core == 0, behind, ahead),
        ("x", "c"),
        [(i * 2 + c, (i + 1 - 2 * c) % 4 * 2 + c) for i in range(4) for c in range(2)],
    )
    other = lax.ppermute(own, "c", [(0, 1), (1, 0)])
    squares = squared(own)
    near = turned(w, ahead, behind)
    far = turned(across)
    place = jnp.stack([core, lax.axis_index("x")]).astype(jnp.int32)
    cosine, sine = tables(length)
    wide = jnp.broadcast_to(gain.reshape(16, shard, 1), (16, shard, 128))
    return block_attention(place, own, other, squares, near, far, wide, cosine, sine)


def solution(mesh):
    fine = Mesh(mesh.devices.reshape(4, 4, 4, 8, 2), ("zh", "x", "y", "zl", "c"))
    split = P(("zh", "x", "y"), ("zl", "c"))
    in_specs = (split, P(), split, split, split)

    return jax.shard_map(local, mesh=fine, in_specs=in_specs, out_specs=split, check_vma=False)
```
